32 devices in a mesh: dp: 16 (over z, x, core), mp: 2 (over y).
Axes of the slice: x: 2, y: 2, z: 4, core: 2. Of those that a mesh axis runs over, the one named last changes fastest.
Arguments:
- tokens: bfloat16 [2560, 1024], P('dp', 'mp'), may hold values from -6 to 6
- slot_embed: bfloat16 [2560, 1024], P('dp', 'mp'), may hold values from -0.1875 to 0.1875
- price_units: int32 [2560], P('dp'), may hold values from 0 to 1535
- unassigned: int32 [2560], P('dp'), may hold values from 0 to 1, as said below
Outputs:
- new_prices: float32 [2560], P(('dp', 'mp'))
- margins: float32 [2560], P('dp')
- unassigned_count: int32 [], replicated
The draws below stay inside these ranges and needn't reach their ends.
Inputs may be any that keep to these rules, and one draw needn't show every extreme that they name: At most 128 of the 160 tokens of each index of dp are unassigned, and some index of dp has exactly 128 in every draw.
All inputs are finite; a program needn't handle non-finite values.
Results may differ from the reference program's by a relative error of at most 0.0004.
Values may be sent and summed in bfloat16 or wider, within the bound.
A program may use at most 128 MiB of HBM per device.

```python
import jax
import jax.numpy as jnp
from jax import lax

D = 1024
TOK_DEV = 160
BUSY = 128
TOKENS = 2560
SLOTS = 2560


def draw_unassigned(key, part):
    groups = TOKENS // TOK_DEV
    floor_count = max(BUSY // 8, 1)
    group_ids = jnp.arange(groups, dtype=jnp.int32)
    base_count = floor_count + (BUSY - floor_count) * (group_ids + 1) * (group_ids + 1) // (groups * groups)
    jitter = jax.random.randint(jax.random.fold_in(key, 11), (groups,), -(floor_count // 2), floor_count // 2 + 1)
    counts = jnp.clip(base_count + jitter, 1, BUSY)
    hot_group = groups - 1 - jax.random.randint(jax.random.fold_in(key, 12), (), 0, max(groups // 4, 1))
    counts = jnp.where(group_ids == hot_group, BUSY, counts)
    noise_bits = jax.random.randint(jax.random.fold_in(key, 13), (groups, TOK_DEV), 0, 1 << 20)
    sort_keys = noise_bits * TOK_DEV + jnp.arange(TOK_DEV, dtype=jnp.int32)[None, :]
    ordering = jnp.argsort(sort_keys, axis=1)
    ranking = jnp.argsort(ordering, axis=1)
    return (ranking < counts[:, None]).astype(jnp.int32).reshape(TOKENS)


def with_ends(entries, key, smallest, high):
    longest = entries.shape.index(max(entries.shape))
    spots = []
    for shift in (0, 1):
        where = [jax.random.randint(jax.random.fold_in(key, axis), (), 0, length) for axis, length in enumerate(entries.shape)]
        where[longest] = (where[longest] + shift) % entries.shape[longest]
        spots.append(tuple(where))
    return entries.at[spots[0]].set(smallest).at[spots[1]].set(high)


def steps_of(key, dims, cuts, low, high):
    def one(position, shards_of):
        draws = jax.random.uniform(jax.random.fold_in(jax.random.fold_in(key, 6), position), (shards_of,), jnp.float32, low / len(cuts), high / len(cuts))
        return jnp.repeat(jnp.exp(draws), dims[position] // shards_of).reshape((-1,) + (1,) * (len(dims) - position - 1))

    loudness = one(*cuts[0])
    for cut in cuts[1:]:
        loudness = loudness * one(*cut)
    return loudness


def gaussian(key, dims, deviation, bound, cuts=(), kind=jnp.bfloat16):
    values = deviation * jax.random.normal(key, dims, jnp.float32)
    if cuts:
        values = values * steps_of(key, dims, cuts, -0.22, 0.18)
    return jnp.clip(values, -bound, bound).astype(kind)


def setup_inputs(seed: int = 0) -> dict:
    key_list = jax.random.split(jax.random.key(seed), 5)
    tokens = gaussian(key_list[0], (TOKENS, D), 1.0, 6.0, ((0, 16), (1, 2)))
    slot_embed = gaussian(key_list[1], (SLOTS, D), D ** -0.5, 0.1875, ((0, 16), (1, 2)))
    price_units = with_ends(jax.random.randint(key_list[2], (SLOTS,), 0, 1536), jax.random.fold_in(key_list[2], 1), 0, 1535).astype(jnp.int32)
    unassigned = draw_unassigned(jax.random.fold_in(key_list[4], 71), 0)
    return dict(tokens=tokens, slot_embed=slot_embed, price_units=price_units, unassigned=unassigned)


unit_price = 1.0 / 512.0


def top_two(values):
    best_value = jnp.max(values, axis=1)
    where_best = jnp.argmax(values, axis=1).astype(jnp.int32)
    column_ids = lax.broadcasted_iota(jnp.int32, values.shape, 1)
    second_value = jnp.max(jnp.where(column_ids == where_best[:, None], -jnp.inf, values), axis=1)
    return best_value, second_value


def reference(tokens, slot_embed, price_units, unassigned):
    prices = price_units.astype(jnp.float32) * unit_price
    groups = TOKENS // TOK_DEV
    token_blocks = tokens.reshape(groups, TOK_DEV, D)
    mask_blocks = unassigned.reshape(groups, TOK_DEV)

    def advance(highest, inputs):
        token_rows, is_live = inputs
        scores = jnp.dot(token_rows, slot_embed.T, preferred_element_type=jnp.float32)
        values = scores - prices[None, :]
        best_value, second_value = top_two(values)
        margin_rows = jnp.where(is_live > 0, best_value - second_value, jnp.float32(0.0))
        excess = jnp.where(is_live[:, None] > 0, values - second_value[:, None], -jnp.inf)
        return jnp.maximum(highest, jnp.max(excess, axis=0)), margin_rows

    initial = jnp.zeros((SLOTS,), jnp.float32)
    highest, margin_blocks = lax.scan(advance, initial, (token_blocks, mask_blocks))
    new_prices = prices + highest
    margins = margin_blocks.reshape(TOKENS)
    unassigned_count = jnp.sum(unassigned).astype(jnp.int32)
    return (new_prices, margins, unassigned_count)
```

```python
import functools

import jax
import jax.numpy as jnp
from jax import lax
from jax.experimental import pallas as pl
from jax.experimental.pallas import tpu as pltpu
from jax.sharding import PartitionSpec as P

MESH = pl.DeviceIdType.MESH
GROUP = 4
LANES = 128

unit_price = 1.0 / 512.0


def loop(low, high, body):
    if high - low <= 8:
        for k in range(low, high):
            body(k)
    else:
        lax.fori_loop(low, high, lambda k, carry: (body(k), carry)[1], 0)


def kernel(
    lines, tok_in, slot_in, price_in, mask_in, prices_out, margins_out, count_out,
    tok, slots, spare, prices, masks, stats, raises, outgoing, vals, best, second,
    load_sem, tok_send, tok_recv, swap_send, right_send, left_send, slot_recv,
    price_send, price_recv, mask_send, mask_recv, stat_send, stat_recv, raise_send, raise_recv,
):
    dp = lax.axis_index("dp")
    y = lax.axis_index("mp")
    yo = 1 - y
    i, z = lax.rem(dp, GROUP), lax.div(dp, GROUP)
    i1 = i + 1 - 2 * lax.rem(i, 2)
    i2 = lax.rem(i + 2, GROUP)
    i3 = GROUP - 1 - i
    half = slots.shape[2]
    own = tok.shape[2]

    def at(ii, zz, yy):
        return {"dp": zz * GROUP + ii, "mp": yy}

    def send(src, dst, send_sem, recv_sem, device):
        return pltpu.make_async_remote_copy(
            src_ref=src, dst_ref=dst, send_sem=send_sem, recv_sem=recv_sem,
            device_id=device, device_id_type=MESH,
        )

    def arrived(dst, recv_sem):
        send(dst, dst, tok_send.at[0], recv_sem, at(i1, z, y)).wait_recv()

    loads = [
        pltpu.make_async_copy(slot_in.at[y], slots.at[y, z], load_sem.at[0]),
        pltpu.make_async_copy(slot_in.at[yo], spare, load_sem.at[1]),
        pltpu.make_async_copy(tok_in, tok.at[y, i], load_sem.at[2]),
        pltpu.make_async_copy(price_in, prices.at[z], load_sem.at[3]),
        pltpu.make_async_copy(mask_in, masks.at[i], load_sem.at[4]),
    ]
    for load in loads:
        load.start()

    plane = [(i1, y), (i2, y), (i3, y), (i, yo), (i1, yo), (i2, yo), (i3, yo)]
    barrier = pltpu.get_barrier_semaphore()
    for ii, yy in plane:
        pl.semaphore_signal(barrier, inc=1, device_id=at(ii, z, yy), device_id_type=MESH)

    def greet(d):
        pl.semaphore_signal(
            barrier, inc=1, device_id=at(i, lax.rem(z + d, lines), y), device_id_type=MESH
        )

    loop(1, lines, greet)
    pl.semaphore_wait(barrier, len(plane) + lines - 1)

    has_right, has_left = z < lines - 1, z > 0

    def to_right(f, zb):
        return send(slots.at[f, zb], slots.at[f, zb], right_send.at[f, zb], slot_recv.at[f, zb],
                    at(i, lax.rem(z + 1, lines), y))

    def to_left(f, zb):
        return send(slots.at[f, zb], slots.at[f, zb], left_send.at[f, zb], slot_recv.at[f, zb],
                    at(i, lax.rem(z + lines - 1, lines), y))

    def send_both(f):
        @pl.when(has_right)
        def _():
            to_right(f, z).start()

        @pl.when(has_left)
        def _():
            to_left(f, z).start()

    loads[0].wait()
    send_both(y)
    loads[1].wait()
    swap = send(spare, slots.at[y, z], swap_send, slot_recv.at[y, z], at(i, z, yo))
    swap.start()
    loads[2].wait()
    mine = tok.at[y, i]
    token_sends = [
        send(mine, mine, tok_send.at[k], tok_recv.at[y, i], device)
        for k, device in enumerate([at(i2, z, y), at(i, z, yo), at(i1, z, y), at(i2, z, yo)])
    ]
    for copy in token_sends:
        copy.start()
    loads[3].wait()
    loads[4].wait()

    def send_price(d):
        send(prices.at[z], prices.at[z], price_send.at[d], price_recv.at[z],
             at(i, lax.rem(z + d, lines), y)).start()

    loop(1, lines, send_price)
    mask_sends = [
        send(masks.at[i], masks.at[i], mask_send.at[k], mask_recv.at[i], at(ii, z, y))
        for k, ii in enumerate([i1, i2, i3])
    ]
    for copy in mask_sends:
        copy.start()

    def relay(d, f):
        @pl.when(has_right & (z - d >= 0))
        def _():
            zb = lax.max(z - d, 0)
            arrived(slots.at[f, zb], slot_recv.at[f, zb])
            to_right(f, zb).start()

        @pl.when(has_left & (z + d < lines))
        def _():
            zb = lax.min(z + d, lines - 1)
            arrived(slots.at[f, zb], slot_recv.at[f, zb])
            to_left(f, zb).start()

    def pass_on(f, ii, k):
        block = tok.at[f, ii]
        arrived(block, tok_recv.at[f, ii])
        copy = send(block, block, tok_send.at[k], tok_recv.at[f, ii], at(i1, z, y))
        copy.start()
        token_sends.append(copy)

    relay(1, y)
    arrived(slots.at[yo, z], slot_recv.at[yo, z])
    send_both(yo)
    pass_on(y, i2, 4)
    relay(1, yo)
    pass_on(yo, i, 5)
    if lines > 2:
        def relay_both(d):
            relay(d, y)
            relay(d, yo)

        loop(2, lines - 1, relay_both)
    pass_on(yo, i2, 6)
    for f, ii in [(y, i1), (y, i3), (yo, i1), (yo, i3)]:
        arrived(tok.at[f, ii], tok_recv.at[f, ii])

    def price_arrived(d):
        zb = lax.rem(z + d, lines)
        arrived(prices.at[zb], price_recv.at[zb])

    loop(1, lines, price_arrived)
    for ii in (i1, i2, i3):
        arrived(masks.at[ii], mask_recv.at[ii])

    best[...] = jnp.full_like(best, -jnp.inf)
    second[...] = jnp.full_like(second, -jnp.inf)

    def price_column(zb):
        row = prices[zb].astype(jnp.float32) * unit_price
        shape = (half, row.shape[1])
        hit = lax.broadcasted_iota(jnp.int32, shape, 1) == lax.broadcasted_iota(jnp.int32, shape, 0) + y * half
        return jnp.sum(jnp.where(hit, row, 0.0), axis=1, keepdims=True)

    def score(zb):
        total = None
        for f in range(2):
            bidders = tok[f].reshape(GROUP * own, tok.shape[3])
            part = lax.dot_general(
                slots[f, zb], bidders, (((1,), (1,)), ((), ())), preferred_element_type=jnp.float32
            )
            total = part if total is None else total + part
        v = total - price_column(zb)
        vals[zb] = v
        b, s = best[...], second[...]
        for k in range(half // 8):
            row = v[8 * k:8 * k + 8]
            s = jnp.maximum(s, jnp.minimum(b, row))
            b = jnp.maximum(b, row)
        best[...] = b
        second[...] = s

    score(z)

    def score_at(d):
        @pl.when(z - d >= 0)
        def _():
            zb = lax.max(z - d, 0)

            @pl.when(jnp.logical_not(has_right))
            def _():
                arrived(slots.at[y, zb], slot_recv.at[y, zb])
                arrived(slots.at[yo, zb], slot_recv.at[yo, zb])

            score(zb)

        @pl.when(z + d < lines)
        def _():
            zb = lax.min(z + d, lines - 1)

            @pl.when(jnp.logical_not(has_left))
            def _():
                arrived(slots.at[y, zb], slot_recv.at[y, zb])
                arrived(slots.at[yo, zb], slot_recv.at[yo, zb])

            score(zb)

    loop(1, lines, score_at)

    b, s = best[...], second[...]
    for shift in (4, 2, 1):
        b2, s2 = pltpu.roll(b, shift, 0), pltpu.roll(s, shift, 0)
        s = jnp.maximum(jnp.minimum(b, b2), jnp.maximum(s, s2))
        b = jnp.maximum(b, b2)
    here = y * GROUP + i
    stats[here, 0:1] = b[0:1]
    stats[here, 1:2] = s[0:1]
    stat_sends = [
        send(stats.at[here], stats.at[here], stat_send.at[k], stat_recv.at[here], at(ii, z, yy))
        for k, (ii, yy) in enumerate(plane)
    ]
    for copy in stat_sends:
        copy.start()

    mask = jnp.concatenate([masks[k] for k in range(GROUP)], axis=1)
    bidders_here = jnp.sum(mask.astype(jnp.float32), axis=1, keepdims=True)

    for ii, yy in plane:
        arrived(stats.at[yy * GROUP + ii], stat_recv.at[yy * GROUP + ii])
    b, s = stats[0, 0:1], stats[0, 1:2]
    for k in range(1, 2 * GROUP):
        b2, s2 = stats[k, 0:1], stats[k, 1:2]
        s = jnp.maximum(jnp.minimum(b, b2), jnp.maximum(s, s2))
        b = jnp.maximum(b, b2)
    bar = jnp.where(mask > 0, s, jnp.inf)

    def excess(d):
        zb = lax.rem(z + d, lines)
        column = jnp.max(vals[zb] - bar, axis=1, keepdims=True)
        shape = (half, LANES)
        hit = lax.broadcasted_iota(jnp.int32, shape, 1) == lax.broadcasted_iota(jnp.int32, shape, 0)
        row = jnp.max(jnp.where(hit, column, -jnp.inf), axis=0, keepdims=True)
        row = jnp.where(lax.broadcasted_iota(jnp.int32, row.shape, 1) == LANES - 1, bidders_here, row)
        return zb, row

    def send_excess(d):
        zb, row = excess(d)
        outgoing[zb] = row
        send(outgoing.at[zb], raises.at[z], raise_send.at[d], raise_recv.at[z], at(i, zb, y)).start()

    loop(1, lines, send_excess)
    raises[z] = excess(0)[1]

    margin = jnp.where(mask > 0, b - s, 0.0)
    mine = margin[:, :own]
    for k in range(1, GROUP):
        mine = jnp.where(i == k, margin[:, k * own:(k + 1) * own], mine)
    margins_out[...] = mine
    units = prices[z].astype(jnp.float32)
    own_prices = jnp.where(y == 0, units[:, :half], units[:, half:2 * half]) * unit_price

    def raise_arrived(d):
        zb = lax.rem(z + d, lines)
        arrived(raises.at[zb], raise_recv.at[zb])

    loop(1, lines, raise_arrived)
    highest, total = raises[0], raises[0]
    for k in range(1, lines):
        highest = jnp.maximum(highest, raises[k])
        total = total + raises[k]
    prices_out[...] = own_prices + jnp.maximum(highest[:, :half], 0.0)
    count_out[...] = total[:, LANES - 1:].astype(jnp.int32)

    swap.wait_send()
    for copy in token_sends + mask_sends + stat_sends:
        copy.wait_send()

    def sent(d):
        zb = lax.rem(z + d, lines)
        send(prices.at[z], prices.at[z], price_send.at[d], price_recv.at[z], at(i, zb, y)).wait_send()
        send(outgoing.at[zb], raises.at[z], raise_send.at[d], raise_recv.at[z], at(i, zb, y)).wait_send()

    loop(1, lines, sent)

    def passed(zb):
        @pl.when(has_right & (zb <= z))
        def _():
            to_right(0, zb).wait_send()
            to_right(1, zb).wait_send()

        @pl.when(has_left & (zb >= z))
        def _():
            to_left(0, zb).wait_send()
            to_left(1, zb).wait_send()

    loop(0, lines, passed)


def on_device(tokens, slot_embed, price_units, unassigned):
    lines = lax.axis_size("dp") // GROUP
    own, width = tokens.shape
    slot_dev = slot_embed.shape[0]
    half = slot_dev // 2
    bidders = GROUP * own
    any_ = pl.BlockSpec(memory_space=pl.ANY)
    vmem = pl.BlockSpec(memory_space=pltpu.VMEM)
    dma = pltpu.SemaphoreType.DMA
    new_prices, margins, total = pl.pallas_call(
        functools.partial(kernel, lines),
        out_shape=(
            jax.ShapeDtypeStruct((1, half), jnp.float32),
            jax.ShapeDtypeStruct((1, own), jnp.float32),
            jax.ShapeDtypeStruct((1, 1), jnp.int32),
        ),
        in_specs=[any_] * 4,
        out_specs=(vmem,) * 3,
        scratch_shapes=[
            pltpu.VMEM((2, GROUP, own, width), jnp.bfloat16),
            pltpu.VMEM((2, lines, half, width), jnp.bfloat16),
            pltpu.VMEM((half, width), jnp.bfloat16),
            pltpu.VMEM((lines, 1, slot_dev), jnp.int32),
            pltpu.VMEM((GROUP, 1, own), jnp.int32),
            pltpu.VMEM((2 * GROUP, 2, bidders), jnp.float32),
            pltpu.VMEM((lines, 1, LANES), jnp.float32),
            pltpu.VMEM((lines, 1, LANES), jnp.float32),
            pltpu.VMEM((lines, half, bidders), jnp.float32),
            pltpu.VMEM((8, bidders), jnp.float32),
            pltpu.VMEM((8, bidders), jnp.float32),
            dma((5,)), dma((7,)), dma((2, GROUP)), dma, dma((2, lines)), dma((2, lines)), dma((2, lines)),
            dma((lines,)), dma((lines,)), dma((3,)), dma((GROUP,)), dma((7,)), dma((2 * GROUP,)),
            dma((lines,)), dma((lines,)),
        ],
        compiler_params=pltpu.CompilerParams(collective_id=0, has_side_effects=True),
        name="auction",
    )(tokens, slot_embed.reshape(2, half, width), price_units.reshape(1, -1), unassigned.reshape(1, -1))
    return new_prices.reshape(-1), margins.reshape(-1), total.reshape(())


def solution(mesh):
    return jax.shard_map(
        on_device,
        mesh=mesh,
        in_specs=(P("dp", "mp"), P("dp", "mp"), P("dp"), P("dp")),
        out_specs=(P(("dp", "mp")), P("dp"), P()),
        check_vma=False,
    )
```

```python
import functools

import jax
import jax.numpy as jnp
from jax import lax
from jax.experimental import pallas as pl
from jax.experimental.pallas import tpu as pltpu
from jax.sharding import PartitionSpec as P

MESH = pl.DeviceIdType.MESH
BUSY = 128
GROUP = 4
LANES = 128

unit_price = 1.0 / 512.0


def loop(low, high, body):
    if high - low <= 8:
        for k in range(low, high):
            body(k)
    else:
        lax.fori_loop(low, high, lambda k, carry: (body(k), carry)[1], 0)


def iota(shape, axis):
    return lax.broadcasted_iota(jnp.int32, shape, axis)


def column_of(row, size):
    shape = (size, row.shape[1])
    return jnp.sum(jnp.where(iota(shape, 1) == iota(shape, 0), row, 0.0), axis=1, keepdims=True)


def keep_two(first, later):
    b, s = first
    b2, s2 = later
    return jnp.maximum(b, b2), jnp.maximum(jnp.minimum(b, b2), jnp.maximum(s, s2))


def kernel(
    lines, cap, tok_in, slot_in, price_in, mask_in, prices_out, margins_out, count_out,
    slot, toks, raw, spare, prices, masks, where_to, cost, stats, raises, outgoing, vals, gaps, halves,
    load_sem, slot_send, slot_recv, swap_send, right_send, left_send, tok_recv,
    price_send, price_recv, stat_send, stat_recv, raise_send, raise_recv, gap_send, gap_recv,
):
    dp = lax.axis_index("dp")
    y = lax.axis_index("mp")
    yo = 1 - y
    i, z = lax.rem(dp, GROUP), lax.div(dp, GROUP)
    i1 = i + 1 - 2 * lax.rem(i, 2)
    i2 = lax.rem(i + 2, GROUP)
    i3 = GROUP - 1 - i
    own = slot.shape[2]
    half = own // 2
    here = y * GROUP + i

    def at(ii, zz, yy):
        return {"dp": zz * GROUP + ii, "mp": yy}

    def send(src, dst, send_sem, recv_sem, device):
        return pltpu.make_async_remote_copy(
            src_ref=src, dst_ref=dst, send_sem=send_sem, recv_sem=recv_sem,
            device_id=device, device_id_type=MESH,
        )

    def arrived(dst, recv_sem):
        send(dst, dst, slot_send.at[0], recv_sem, at(i1, z, y)).wait_recv()

    loads = [
        pltpu.make_async_copy(mask_in, masks, load_sem.at[0]),
        pltpu.make_async_copy(tok_in, raw, load_sem.at[1]),
        pltpu.make_async_copy(slot_in, slot.at[y, i], load_sem.at[2]),
        pltpu.make_async_copy(price_in, prices.at[i], load_sem.at[3]),
    ]
    for load in loads:
        load.start()

    has_right, has_left = z < lines - 1, z > 0
    plane = [(i1, y), (i2, y), (i3, y), (i, yo), (i1, yo), (i2, yo), (i3, yo)]
    barrier = pltpu.get_barrier_semaphore()
    for ii, yy in plane:
        pl.semaphore_signal(barrier, inc=1, device_id=at(ii, z, yy), device_id_type=MESH)

    @pl.when(has_right)
    def _():
        pl.semaphore_signal(barrier, inc=1, device_id=at(i, z + 1, y), device_id_type=MESH)

    @pl.when(has_left)
    def _():
        pl.semaphore_signal(barrier, inc=1, device_id=at(i, z - 1, y), device_id_type=MESH)

    loads[0].wait()
    live = masks[...] > 0
    ones = jnp.broadcast_to(jnp.where(live, 1.0, 0.0), (8, own)).astype(jnp.bfloat16)
    before = jnp.where(iota((own, own), 0) < iota((own, own), 1), 1.0, 0.0).astype(jnp.bfloat16)
    place = jnp.dot(ones, before, preferred_element_type=jnp.float32)[0:1]
    place = jnp.where(live, place, -1.0)
    where_to[...] = place
    busy = jnp.sum(jnp.where(live, 1.0, 0.0), axis=1, keepdims=True)
    hits = place == iota((2 * cap, own), 0).astype(jnp.float32)
    hits = jnp.where(hits, 1.0, 0.0).astype(jnp.bfloat16)
    loads[1].wait()
    packed = jnp.dot(hits, raw[...], preferred_element_type=jnp.float32).astype(jnp.bfloat16)
    low, high = packed[:cap], packed[cap:]
    toks[y, z] = jnp.where(y == 0, low, high)
    spare[...] = jnp.where(y == 0, high, low)

    @pl.when(has_right & has_left)
    def _():
        pl.semaphore_wait(barrier, len(plane) + 2)

    @pl.when(jnp.logical_not(has_right & has_left))
    def _():
        pl.semaphore_wait(barrier, len(plane) + min(lines - 1, 1))

    def to_right(f, zb):
        return send(toks.at[f, zb], toks.at[f, zb], right_send.at[f, zb], tok_recv.at[f, zb],
                    at(i, lax.rem(z + 1, lines), y))

    def to_left(f, zb):
        return send(toks.at[f, zb], toks.at[f, zb], left_send.at[f, zb], tok_recv.at[f, zb],
                    at(i, lax.rem(z + lines - 1, lines), y))

    def send_both(f):
        @pl.when(has_right)
        def _():
            to_right(f, z).start()

        @pl.when(has_left)
        def _():
            to_left(f, z).start()

    swap = send(spare, toks.at[y, z], swap_send, tok_recv.at[y, z], at(i, z, yo))
    swap.start()
    send_both(y)
    loads[2].wait()
    mine = slot.at[y, i]
    slot_sends = [
        send(mine, mine, slot_send.at[k], slot_recv.at[y, i], device)
        for k, device in enumerate([at(i2, z, y), at(i, z, yo), at(i1, z, y), at(i2, z, yo)])
    ]
    for copy in slot_sends:
        copy.start()
    loads[3].wait()
    price_sends = [
        send(prices.at[i], prices.at[i], price_send.at[k], price_recv.at[i], at(ii, z, y))
        for k, ii in enumerate([i1, i2, i3])
    ]
    for copy in price_sends:
        copy.start()

    def relay(d, f):
        @pl.when(has_right & (z - d >= 0))
        def _():
            zb = lax.max(z - d, 0)
            arrived(toks.at[f, zb], tok_recv.at[f, zb])
            to_right(f, zb).start()

        @pl.when(has_left & (z + d < lines))
        def _():
            zb = lax.min(z + d, lines - 1)
            arrived(toks.at[f, zb], tok_recv.at[f, zb])
            to_left(f, zb).start()

    def pass_on(f, ii, k):
        block = slot.at[f, ii]
        arrived(block, slot_recv.at[f, ii])
        copy = send(block, block, slot_send.at[k], slot_recv.at[f, ii], at(i1, z, y))
        copy.start()
        slot_sends.append(copy)

    arrived(toks.at[yo, z], tok_recv.at[yo, z])
    send_both(yo)
    relay(1, y)
    pass_on(y, i2, 4)
    relay(1, yo)
    pass_on(yo, i, 5)
    if lines > 2:
        def relay_both(d):
            relay(d, y)
            relay(d, yo)

        loop(2, lines - 1, relay_both)
    for ii in (i1, i2, i3):
        arrived(prices.at[ii], price_recv.at[ii])
    for k in range(GROUP):
        column = column_of(prices[k].astype(jnp.float32) * unit_price, own)
        cost[k * own:(k + 1) * own] = jnp.broadcast_to(column, (own, cap))
    pass_on(yo, i2, 6)
    for f, ii in [(y, i1), (y, i3), (yo, i1), (yo, i3)]:
        arrived(slot.at[f, ii], slot_recv.at[f, ii])

    def score(zb):
        total = None
        for f in range(2):
            rows = slot[f].reshape(GROUP * own, slot.shape[3])
            part = lax.dot_general(
                rows, toks[f, zb], (((1,), (1,)), ((), ())), preferred_element_type=jnp.float32
            )
            total = part if total is None else total + part
        v = total - cost[...]
        vals[zb] = v
        step = 32
        b, s = v[:step], jnp.full((step, cap), -jnp.inf)
        for k in range(1, GROUP * own // step):
            row = v[step * k:step * (k + 1)]
            s = jnp.maximum(s, jnp.minimum(b, row))
            b = jnp.maximum(b, row)
        while step > 8:
            step //= 2
            b, s = keep_two((b[:step], s[:step]), (b[step:], s[step:]))
        for shift in (4, 2, 1):
            b, s = keep_two((b, s), (pltpu.roll(b, shift, 0), pltpu.roll(s, shift, 0)))
        stats[z, pl.ds(zb, 1)] = jnp.concatenate([b[0:1], s[0:1]], axis=1)

    score(z)

    def score_at(d):
        @pl.when(z - d >= 0)
        def _():
            zb = lax.max(z - d, 0)

            @pl.when(jnp.logical_not(has_right))
            def _():
                arrived(toks.at[y, zb], tok_recv.at[y, zb])
                arrived(toks.at[yo, zb], tok_recv.at[yo, zb])

            score(zb)

        @pl.when(z + d < lines)
        def _():
            zb = lax.min(z + d, lines - 1)

            @pl.when(jnp.logical_not(has_left))
            def _():
                arrived(toks.at[y, zb], tok_recv.at[y, zb])
                arrived(toks.at[yo, zb], tok_recv.at[yo, zb])

            score(zb)

    stats[z, lines:] = jnp.broadcast_to(busy, (lines, LANES))
    loop(1, lines, score_at)

    def stat_to(d):
        return send(stats.at[z], stats.at[z], stat_send.at[d], stat_recv.at[z], at(i, lax.rem(z + d, lines), y))

    loop(1, lines, lambda d: stat_to(d).start())

    def stat_arrived(d):
        zb = lax.rem(z + d, lines)
        arrived(stats.at[zb], stat_recv.at[zb])

    loop(1, lines, stat_arrived)
    b, s = stats[0, :lines, :cap], stats[0, :lines, cap:]
    for k in range(1, lines):
        b, s = keep_two((b, s), (stats[k, :lines, :cap], stats[k, :lines, cap:]))
    number = y * cap + iota((1, cap), 1)
    top, bidders = None, None
    for k in range(lines):
        count = stats[k, lines:lines + 1, :cap]
        valid = number.astype(jnp.float32) < count
        gaps[k] = jnp.where(valid, b[k:k + 1] - s[k:k + 1], 0.0)
        excess = vals[k] - jnp.where(valid, s[k:k + 1], jnp.inf)
        top = excess if top is None else jnp.maximum(top, excess)
        bidders = count if bidders is None else bidders + count
    bidders = bidders[:, :1]
    halves[y] = gaps[z]
    gap_to = send(halves.at[y], halves.at[y], gap_send, gap_recv, at(i, z, yo))
    gap_to.start()

    def raise_to(k):
        return send(outgoing.at[k], raises.at[here], raise_send.at[k], raise_recv.at[here],
                    at(k % GROUP, z, k // GROUP))

    for k in range(2 * GROUP):
        first = (k % GROUP) * own + (k // GROUP) * half
        column = jnp.max(top[first:first + half], axis=1, keepdims=True)
        shape = (half, LANES)
        row = jnp.max(jnp.where(iota(shape, 1) == iota(shape, 0), column, -jnp.inf), axis=0, keepdims=True)
        outgoing[k] = jnp.where(iota(row.shape, 1) == LANES - 1, bidders, row)

        @pl.when(here != k)
        def _():
            raise_to(k).start()

    raises[here] = outgoing[here]
    units = prices[i].astype(jnp.float32)
    own_prices = jnp.where(y == 0, units[:, :half], units[:, half:2 * half]) * unit_price

    arrived(halves.at[yo], gap_recv)
    both = jnp.concatenate([halves[0], halves[1]], axis=1)
    hit = where_to[...] == iota((2 * cap, own), 0).astype(jnp.float32)
    margins_out[...] = jnp.sum(jnp.where(hit, column_of(both, 2 * cap), 0.0), axis=0, keepdims=True)

    for ii, yy in plane:
        arrived(raises.at[yy * GROUP + ii], raise_recv.at[yy * GROUP + ii])
    highest, total = raises[0], raises[0]
    for k in range(1, 2 * GROUP):
        highest = jnp.maximum(highest, raises[k])
        total = total + raises[k]
    prices_out[...] = own_prices + jnp.maximum(highest[:, :half], 0.0)
    count_out[...] = (total[:, LANES - 1:] * 0.5).astype(jnp.int32)

    swap.wait_send()
    gap_to.wait_send()
    for copy in slot_sends + price_sends:
        copy.wait_send()
    loop(1, lines, lambda d: stat_to(d).wait_send())
    for k in range(2 * GROUP):
        @pl.when(here != k)
        def _():
            raise_to(k).wait_send()

    def passed(zb):
        @pl.when(has_right & (zb <= z))
        def _():
            to_right(0, zb).wait_send()
            to_right(1, zb).wait_send()

        @pl.when(has_left & (zb >= z))
        def _():
            to_left(0, zb).wait_send()
            to_left(1, zb).wait_send()

    loop(0, lines, passed)


def on_device(tokens, slot_embed, price_units, unassigned):
    lines = lax.axis_size("dp") // GROUP
    own, width = tokens.shape
    half, cap = own // 2, BUSY // 2
    every = GROUP * own
    any_ = pl.BlockSpec(memory_space=pl.ANY)
    vmem = pl.BlockSpec(memory_space=pltpu.VMEM)
    dma = pltpu.SemaphoreType.DMA
    new_prices, margins, total = pl.pallas_call(
        functools.partial(kernel, lines, cap),
        out_shape=(
            pltpu.VMEM((1, half), jnp.float32),
            pltpu.VMEM((1, own), jnp.float32),
            pltpu.VMEM((1, 1), jnp.int32),
        ),
        in_specs=[any_] * 4,
        out_specs=(vmem,) * 3,
        scratch_shapes=[
            pltpu.VMEM((2, GROUP, own, width), jnp.bfloat16),
            pltpu.VMEM((2, lines, cap, width), jnp.bfloat16),
            pltpu.VMEM((own, width), jnp.bfloat16),
            pltpu.VMEM((cap, width), jnp.bfloat16),
            pltpu.VMEM((GROUP, 1, own), jnp.int32),
            pltpu.VMEM((1, own), jnp.int32),
            pltpu.VMEM((1, own), jnp.float32),
            pltpu.VMEM((every, cap), jnp.float32),
            pltpu.VMEM((lines, 2 * lines, LANES), jnp.float32),
            pltpu.VMEM((2 * GROUP, 1, LANES), jnp.float32),
            pltpu.VMEM((2 * GROUP, 1, LANES), jnp.float32),
            pltpu.VMEM((lines, every, cap), jnp.float32),
            pltpu.VMEM((lines, 1, cap), jnp.float32),
            pltpu.VMEM((2, 1, cap), jnp.float32),
            dma((4,)), dma((7,)), dma((2, GROUP)), dma, dma((2, lines)), dma((2, lines)), dma((2, lines)),
            dma((3,)), dma((GROUP,)), dma((lines,)), dma((lines,)), dma((2 * GROUP,)), dma((2 * GROUP,)), dma, dma,
        ],
        compiler_params=pltpu.CompilerParams(collective_id=0, has_side_effects=True),
        name="auction",
    )(tokens, slot_embed, price_units.reshape(1, -1), unassigned.reshape(1, -1))
    return new_prices.reshape(-1), margins.reshape(-1), total.reshape(())


def solution(mesh):
    return jax.shard_map(
        on_device,
        mesh=mesh,
        in_specs=(P("dp", "mp"), P("dp", "mp"), P("dp"), P("dp")),
        out_specs=(P(("dp", "mp")), P("dp"), P()),
        check_vma=False,
    )
```

```python
import functools

import jax
import jax.numpy as jnp
from jax import lax
from jax.experimental import pallas as pl
from jax.experimental.pallas import tpu as pltpu
from jax.sharding import PartitionSpec as P

MESH = pl.DeviceIdType.MESH
BUSY = 128
GROUP = 4
LANES = 128

unit_price = 1.0 / 512.0


def loop(low, high, body):
    if high - low <= 8:
        for k in range(low, high):
            body(k)
    else:
        lax.fori_loop(low, high, lambda k, carry: (body(k), carry)[1], 0)


def iota(shape, axis):
    return lax.broadcasted_iota(jnp.int32, shape, axis)


def column_of(row, size):
    shape = (size, row.shape[1])
    return jnp.sum(jnp.where(iota(shape, 1) == iota(shape, 0), row, 0.0), axis=1, keepdims=True)


def keep_two(first, later):
    b, s = first
    b2, s2 = later
    return jnp.maximum(b, b2), jnp.maximum(jnp.minimum(b, b2), jnp.maximum(s, s2))


def kernel(
    lines, cap, tok_in, slot_in, price_in, mask_in, prices_out, margins_out, count_out,
    slot, toks, raw, spare, prices, masks, where_to, cost, stats, raises, outgoing, vals, gaps, halves,
    load_sem, slot_send, slot_recv, swap_send, right_send, left_send, tok_recv,
    price_send, price_recv, stat_send, stat_recv, raise_send, raise_recv, gap_send, gap_recv,
):
    dp = lax.axis_index("dp")
    y = lax.axis_index("mp")
    yo = 1 - y
    i, z = lax.rem(dp, GROUP), lax.div(dp, GROUP)
    i1 = i + 1 - 2 * lax.rem(i, 2)
    i2 = lax.rem(i + 2, GROUP)
    i3 = GROUP - 1 - i
    own = slot.shape[2]
    half = own // 2
    here = y * GROUP + i

    def at(ii, zz, yy):
        return {"dp": zz * GROUP + ii, "mp": yy}

    def send(src, dst, send_sem, recv_sem, device):
        return pltpu.make_async_remote_copy(
            src_ref=src, dst_ref=dst, send_sem=send_sem, recv_sem=recv_sem,
            device_id=device, device_id_type=MESH,
        )

    def arrived(dst, recv_sem):
        send(dst, dst, slot_send.at[0], recv_sem, at(i1, z, y)).wait_recv()

    loads = [
        pltpu.make_async_copy(mask_in, masks, load_sem.at[0]),
        pltpu.make_async_copy(tok_in, raw, load_sem.at[1]),
        pltpu.make_async_copy(slot_in, slot.at[y, i], load_sem.at[2]),
        pltpu.make_async_copy(price_in, prices.at[i], load_sem.at[3]),
    ]
    for load in loads:
        load.start()

    has_right, has_left = z < lines - 1, z > 0
    plane = [(i1, y), (i2, y), (i3, y), (i, yo), (i1, yo), (i2, yo), (i3, yo)]
    barrier = pltpu.get_barrier_semaphore()
    for ii, yy in plane:
        pl.semaphore_signal(barrier, inc=1, device_id=at(ii, z, yy), device_id_type=MESH)

    @pl.when(has_right)
    def _():
        pl.semaphore_signal(barrier, inc=1, device_id=at(i, z + 1, y), device_id_type=MESH)

    @pl.when(has_left)
    def _():
        pl.semaphore_signal(barrier, inc=1, device_id=at(i, z - 1, y), device_id_type=MESH)

    loads[0].wait()
    live = masks[...] > 0
    ones = jnp.broadcast_to(jnp.where(live, 1.0, 0.0), (8, own)).astype(jnp.bfloat16)
    before = jnp.where(iota((own, own), 0) < iota((own, own), 1), 1.0, 0.0).astype(jnp.bfloat16)
    place = jnp.dot(ones, before, preferred_element_type=jnp.float32)[0:1]
    place = jnp.where(live, place, -1.0)
    where_to[...] = place
    busy = jnp.sum(jnp.where(live, 1.0, 0.0), axis=1, keepdims=True)
    hits = place == iota((2 * cap, own), 0).astype(jnp.float32)
    hits = jnp.where(hits, 1.0, 0.0).astype(jnp.bfloat16)
    loads[1].wait()
    packed = jnp.dot(hits, raw[...], preferred_element_type=jnp.float32).astype(jnp.bfloat16)
    low, high = packed[:cap], packed[cap:]
    toks[y, z] = jnp.where(y == 0, low, high)
    spare[...] = jnp.where(y == 0, high, low)

    @pl.when(has_right & has_left)
    def _():
        pl.semaphore_wait(barrier, len(plane) + 2)

    @pl.when(jnp.logical_not(has_right & has_left))
    def _():
        pl.semaphore_wait(barrier, len(plane) + min(lines - 1, 1))

    def to_right(f, zb, q):
        block = tok_part(f, zb, q)
        return send(block, block, right_send.at[f, zb, q], tok_recv.at[f, zb, q], at(i, lax.rem(z + 1, lines), y))

    def to_left(f, zb, q):
        block = tok_part(f, zb, q)
        return send(block, block, left_send.at[f, zb, q], tok_recv.at[f, zb, q],
                    at(i, lax.rem(z + lines - 1, lines), y))

    def tok_part(f, zb, q):
        rows = toks.shape[2] // 2
        return toks.at[f, zb, pl.ds(q * rows, rows)]

    def slot_part(f, ii, q):
        return slot.at[f, ii, pl.ds(q * half, half)]

    def tok_arrived(f, zb, q):
        arrived(tok_part(f, zb, q), tok_recv.at[f, zb, q])

    def slot_arrived(f, ii, q):
        arrived(slot_part(f, ii, q), slot_recv.at[f, ii, q])

    def send_both(f, q):
        @pl.when(has_right)
        def _():
            to_right(f, z, q).start()

        @pl.when(has_left)
        def _():
            to_left(f, z, q).start()

    swaps = [
        send(spare.at[pl.ds(q * (cap // 2), cap // 2)], tok_part(y, z, q), swap_send.at[q], tok_recv.at[y, z, q],
             at(i, z, yo))
        for q in range(2)
    ]
    for q in range(2):
        swaps[q].start()
        send_both(y, q)
    slot_sends = []

    def send_slots(f, ii, q, device):
        block = slot_part(f, ii, q)
        copy = send(block, block, slot_send.at[len(slot_sends)], slot_recv.at[f, ii, q], device)
        copy.start()
        slot_sends.append(copy)

    loads[2].wait()
    for device in (at(i2, z, y), at(i, z, yo), at(i1, z, y)):
        for q in range(2):
            send_slots(y, i, q, device)
    loads[3].wait()
    price_sends = [
        send(prices.at[i], prices.at[i], price_send.at[k], price_recv.at[i], at(ii, z, y))
        for k, ii in enumerate([i1, i2, i3])
    ]
    for copy in price_sends:
        copy.start()

    def relay(d, f, q):
        @pl.when(has_right & (z - d >= 0))
        def _():
            zb = lax.max(z - d, 0)
            tok_arrived(f, zb, q)
            to_right(f, zb, q).start()

        @pl.when(has_left & (z + d < lines))
        def _():
            zb = lax.min(z + d, lines - 1)
            tok_arrived(f, zb, q)
            to_left(f, zb, q).start()

    beside, across, over = at(i1, z, y), at(i2, z, y), at(i, z, yo)
    for q in range(2):
        tok_arrived(yo, z, q)
        send_both(yo, q)
        relay(1, y, q)
    slot_arrived(y, i2, 0)
    send_slots(y, i2, 0, beside)
    relay(1, yo, 0)
    slot_arrived(yo, i, 0)
    send_slots(yo, i, 0, across)
    send_slots(yo, i, 0, beside)
    slot_arrived(y, i2, 1)
    send_slots(y, i2, 1, over)
    send_slots(y, i2, 1, beside)
    relay(1, yo, 1)
    if lines > 3:
        for q in range(2):
            relay(2, y, q)
    slot_arrived(yo, i, 1)
    send_slots(yo, i, 1, beside)
    if lines > 3:
        for q in range(2):
            relay(2, yo, q)

        def relay_all(d):
            for f in (y, yo):
                for q in range(2):
                    relay(d, f, q)

        loop(3, lines - 1, relay_all)
    for ii in (i1, i2, i3):
        arrived(prices.at[ii], price_recv.at[ii])
    for k in range(GROUP):
        column = column_of(prices[k].astype(jnp.float32) * unit_price, own)
        cost[k * own:(k + 1) * own] = jnp.broadcast_to(column, (own, cap))
    for q in range(2):
        slot_arrived(yo, i2, q)
        send_slots(yo, i2, q, beside)
    for f, ii in [(y, i1), (y, i3), (yo, i1), (yo, i3)]:
        for q in range(2):
            slot_arrived(f, ii, q)

    def score(zb):
        total = None
        for f in range(2):
            rows = slot[f].reshape(GROUP * own, slot.shape[3])
            part = lax.dot_general(
                rows, toks[f, zb], (((1,), (1,)), ((), ())), preferred_element_type=jnp.float32
            )
            total = part if total is None else total + part
        v = total - cost[...]
        vals[zb] = v
        step = 32
        b, s = v[:step], jnp.full((step, cap), -jnp.inf)
        for k in range(1, GROUP * own // step):
            row = v[step * k:step * (k + 1)]
            s = jnp.maximum(s, jnp.minimum(b, row))
            b = jnp.maximum(b, row)
        while step > 8:
            step //= 2
            b, s = keep_two((b[:step], s[:step]), (b[step:], s[step:]))
        for shift in (4, 2, 1):
            b, s = keep_two((b, s), (pltpu.roll(b, shift, 0), pltpu.roll(s, shift, 0)))
        stats[z, pl.ds(zb, 1)] = jnp.concatenate([b[0:1], s[0:1]], axis=1)

    score(z)

    def score_at(d):
        @pl.when(z - d >= 0)
        def _():
            zb = lax.max(z - d, 0)

            @pl.when(jnp.logical_not(has_right))
            def _():
                for q in range(2):
                    tok_arrived(y, zb, q)
                    tok_arrived(yo, zb, q)

            score(zb)

        @pl.when(z + d < lines)
        def _():
            zb = lax.min(z + d, lines - 1)

            @pl.when(jnp.logical_not(has_left))
            def _():
                for q in range(2):
                    tok_arrived(y, zb, q)
                    tok_arrived(yo, zb, q)

            score(zb)

    stats[z, lines:] = jnp.broadcast_to(busy, (lines, LANES))
    loop(1, lines, score_at)

    def stat_to(d):
        return send(stats.at[z], stats.at[z], stat_send.at[d], stat_recv.at[z], at(i, lax.rem(z + d, lines), y))

    loop(1, lines, lambda d: stat_to(d).start())

    def stat_arrived(d):
        zb = lax.rem(z + d, lines)
        arrived(stats.at[zb], stat_recv.at[zb])

    loop(1, lines, stat_arrived)
    b, s = stats[0, :lines, :cap], stats[0, :lines, cap:]
    for k in range(1, lines):
        b, s = keep_two((b, s), (stats[k, :lines, :cap], stats[k, :lines, cap:]))
    number = y * cap + iota((1, cap), 1)
    top, bidders = None, None
    for k in range(lines):
        count = stats[k, lines:lines + 1, :cap]
        valid = number.astype(jnp.float32) < count
        gaps[k] = jnp.where(valid, b[k:k + 1] - s[k:k + 1], 0.0)
        excess = vals[k] - jnp.where(valid, s[k:k + 1], jnp.inf)
        top = excess if top is None else jnp.maximum(top, excess)
        bidders = count if bidders is None else bidders + count
    bidders = bidders[:, :1]
    halves[y] = gaps[z]
    gap_to = send(halves.at[y], halves.at[y], gap_send, gap_recv, at(i, z, yo))
    gap_to.start()

    def raise_to(k):
        return send(outgoing.at[k], raises.at[here], raise_send.at[k], raise_recv.at[here],
                    at(k % GROUP, z, k // GROUP))

    for k in range(2 * GROUP):
        first = (k % GROUP) * own + (k // GROUP) * half
        column = jnp.max(top[first:first + half], axis=1, keepdims=True)
        shape = (half, LANES)
        row = jnp.max(jnp.where(iota(shape, 1) == iota(shape, 0), column, -jnp.inf), axis=0, keepdims=True)
        outgoing[k] = jnp.where(iota(row.shape, 1) == LANES - 1, bidders, row)

        @pl.when(here != k)
        def _():
            raise_to(k).start()

    raises[here] = outgoing[here]
    units = prices[i].astype(jnp.float32)
    own_prices = jnp.where(y == 0, units[:, :half], units[:, half:2 * half]) * unit_price

    arrived(halves.at[yo], gap_recv)
    both = jnp.concatenate([halves[0], halves[1]], axis=1)
    hit = where_to[...] == iota((2 * cap, own), 0).astype(jnp.float32)
    margins_out[...] = jnp.sum(jnp.where(hit, column_of(both, 2 * cap), 0.0), axis=0, keepdims=True)

    for ii, yy in plane:
        arrived(raises.at[yy * GROUP + ii], raise_recv.at[yy * GROUP + ii])
    highest, total = raises[0], raises[0]
    for k in range(1, 2 * GROUP):
        highest = jnp.maximum(highest, raises[k])
        total = total + raises[k]
    prices_out[...] = own_prices + jnp.maximum(highest[:, :half], 0.0)
    count_out[...] = (total[:, LANES - 1:] * 0.5).astype(jnp.int32)

    gap_to.wait_send()
    for copy in swaps + slot_sends + price_sends:
        copy.wait_send()
    loop(1, lines, lambda d: stat_to(d).wait_send())
    for k in range(2 * GROUP):
        @pl.when(here != k)
        def _():
            raise_to(k).wait_send()

    pieces = [(f, q) for f in range(2) for q in range(2)]

    def passed(zb):
        @pl.when(has_right & (zb <= z))
        def _():
            for f, q in pieces:
                to_right(f, zb, q).wait_send()

        @pl.when(has_left & (zb >= z))
        def _():
            for f, q in pieces:
                to_left(f, zb, q).wait_send()

    loop(0, lines, passed)


def on_device(tokens, slot_embed, price_units, unassigned):
    lines = lax.axis_size("dp") // GROUP
    own, width = tokens.shape
    half, cap = own // 2, BUSY // 2
    every = GROUP * own
    any_ = pl.BlockSpec(memory_space=pl.ANY)
    vmem = pl.BlockSpec(memory_space=pltpu.VMEM)
    dma = pltpu.SemaphoreType.DMA
    new_prices, margins, total = pl.pallas_call(
        functools.partial(kernel, lines, cap),
        out_shape=(
            pltpu.VMEM((1, half), jnp.float32),
            pltpu.VMEM((1, own), jnp.float32),
            pltpu.VMEM((1, 1), jnp.int32),
        ),
        in_specs=[any_] * 4,
        out_specs=(vmem,) * 3,
        scratch_shapes=[
            pltpu.VMEM((2, GROUP, own, width), jnp.bfloat16),
            pltpu.VMEM((2, lines, cap, width), jnp.bfloat16),
            pltpu.VMEM((own, width), jnp.bfloat16),
            pltpu.VMEM((cap, width), jnp.bfloat16),
            pltpu.VMEM((GROUP, 1, own), jnp.int32),
            pltpu.VMEM((1, own), jnp.int32),
            pltpu.VMEM((1, own), jnp.float32),
            pltpu.VMEM((every, cap), jnp.float32),
            pltpu.VMEM((lines, 2 * lines, LANES), jnp.float32),
            pltpu.VMEM((2 * GROUP, 1, LANES), jnp.float32),
            pltpu.VMEM((2 * GROUP, 1, LANES), jnp.float32),
            pltpu.VMEM((lines, every, cap), jnp.float32),
            pltpu.VMEM((lines, 1, cap), jnp.float32),
            pltpu.VMEM((2, 1, cap), jnp.float32),
            dma((4,)), dma((14,)), dma((2, GROUP, 2)), dma((2,)), dma((2, lines, 2)), dma((2, lines, 2)),
            dma((2, lines, 2)),
            dma((3,)), dma((GROUP,)), dma((lines,)), dma((lines,)), dma((2 * GROUP,)), dma((2 * GROUP,)), dma, dma,
        ],
        compiler_params=pltpu.CompilerParams(collective_id=0, has_side_effects=True),
        name="auction",
    )(tokens, slot_embed, price_units.reshape(1, -1), unassigned.reshape(1, -1))
    return new_prices.reshape(-1), margins.reshape(-1), total.reshape(())


def solution(mesh):
    return jax.shard_map(
        on_device,
        mesh=mesh,
        in_specs=(P("dp", "mp"), P("dp", "mp"), P("dp"), P("dp")),
        out_specs=(P(("dp", "mp")), P("dp"), P()),
        check_vma=False,
    )
```

```python
import functools

import jax
import jax.numpy as jnp
from jax import lax
from jax.experimental import pallas as pl
from jax.experimental.pallas import tpu as pltpu
from jax.sharding import PartitionSpec as P

MESH = pl.DeviceIdType.MESH
BUSY = 128
GROUP = 4
LANES = 128

unit_price = 1.0 / 512.0


def loop(low, high, body):
    if high - low <= 8:
        for k in range(low, high):
            body(k)
    else:
        lax.fori_loop(low, high, lambda k, carry: (body(k), carry)[1], 0)


def iota(shape, axis):
    return lax.broadcasted_iota(jnp.int32, shape, axis)


def column_of(row, size):
    shape = (size, row.shape[1])
    return jnp.sum(jnp.where(iota(shape, 1) == iota(shape, 0), row, 0.0), axis=1, keepdims=True)


def keep_two(first, later):
    b, s = first
    b2, s2 = later
    return jnp.maximum(b, b2), jnp.maximum(jnp.minimum(b, b2), jnp.maximum(s, s2))


def kernel(
    lines, cap, tok_in, slot_in, price_in, mask_in, prices_out, margins_out, count_out,
    slot, toks, raw, spare, prices, masks, where_to, cost, stats, raises, outgoing, vals, gaps, halves,
    load_sem, slot_send, slot_recv, swap_send, right_send, left_send, tok_recv,
    price_send, price_recv, stat_send, stat_recv, raise_send, raise_recv, gap_send, gap_recv,
):
    dp = lax.axis_index("dp")
    y = lax.axis_index("mp")
    yo = 1 - y
    i, z = lax.rem(dp, GROUP), lax.div(dp, GROUP)
    i1 = i + 1 - 2 * lax.rem(i, 2)
    i2 = lax.rem(i + 2, GROUP)
    i3 = GROUP - 1 - i
    own = slot.shape[2]
    half = own // 2
    here = y * GROUP + i

    def at(ii, zz, yy):
        return {"dp": zz * GROUP + ii, "mp": yy}

    def send(src, dst, send_sem, recv_sem, device):
        return pltpu.make_async_remote_copy(
            src_ref=src, dst_ref=dst, send_sem=send_sem, recv_sem=recv_sem,
            device_id=device, device_id_type=MESH,
        )

    def arrived(dst, recv_sem):
        send(dst, dst, slot_send.at[0], recv_sem, at(i1, z, y)).wait_recv()

    loads = [
        pltpu.make_async_copy(mask_in, masks, load_sem.at[0]),
        pltpu.make_async_copy(tok_in, raw, load_sem.at[1]),
        pltpu.make_async_copy(slot_in, slot.at[y, i], load_sem.at[2]),
        pltpu.make_async_copy(price_in, prices.at[i], load_sem.at[3]),
    ]
    for load in loads:
        load.start()

    has_right, has_left = z < lines - 1, z > 0
    plane = [(i1, y), (i2, y), (i3, y), (i, yo), (i1, yo), (i2, yo), (i3, yo)]
    barrier = pltpu.get_barrier_semaphore()
    for ii, yy in plane:
        pl.semaphore_signal(barrier, inc=1, device_id=at(ii, z, yy), device_id_type=MESH)

    @pl.when(has_right)
    def _():
        pl.semaphore_signal(barrier, inc=1, device_id=at(i, z + 1, y), device_id_type=MESH)

    @pl.when(has_left)
    def _():
        pl.semaphore_signal(barrier, inc=1, device_id=at(i, z - 1, y), device_id_type=MESH)

    loads[0].wait()
    live = masks[...] > 0
    ones = jnp.broadcast_to(jnp.where(live, 1.0, 0.0), (8, own)).astype(jnp.bfloat16)
    before = jnp.where(iota((own, own), 0) < iota((own, own), 1), 1.0, 0.0).astype(jnp.bfloat16)
    place = jnp.dot(ones, before, preferred_element_type=jnp.float32)[0:1]
    place = jnp.where(live, place, -1.0)
    where_to[...] = place
    busy = jnp.sum(jnp.where(live, 1.0, 0.0), axis=1, keepdims=True)
    hits = place == iota((2 * cap, own), 0).astype(jnp.float32)
    hits = jnp.where(hits, 1.0, 0.0).astype(jnp.bfloat16)
    loads[1].wait()
    packed = jnp.dot(hits, raw[...], preferred_element_type=jnp.float32).astype(jnp.bfloat16)
    low, high = packed[:cap], packed[cap:]
    toks[y, z] = jnp.where(y == 0, low, high)
    spare[...] = jnp.where(y == 0, high, low)

    @pl.when(has_right & has_left)
    def _():
        pl.semaphore_wait(barrier, len(plane) + 2)

    @pl.when(jnp.logical_not(has_right & has_left))
    def _():
        pl.semaphore_wait(barrier, len(plane) + min(lines - 1, 1))

    def to_right(f, zb, q):
        block = tok_part(f, zb, q)
        return send(block, block, right_send.at[f, zb, q], tok_recv.at[f, zb, q], at(i, lax.rem(z + 1, lines), y))

    def to_left(f, zb, q):
        block = tok_part(f, zb, q)
        return send(block, block, left_send.at[f, zb, q], tok_recv.at[f, zb, q],
                    at(i, lax.rem(z + lines - 1, lines), y))

    def tok_part(f, zb, q):
        rows = toks.shape[2] // 2
        return toks.at[f, zb, pl.ds(q * rows, rows)]

    def slot_part(f, ii, q):
        return slot.at[f, ii, pl.ds(q * half, half)]

    def tok_arrived(f, zb, q):
        arrived(tok_part(f, zb, q), tok_recv.at[f, zb, q])

    def slot_arrived(f, ii, q):
        arrived(slot_part(f, ii, q), slot_recv.at[f, ii, q])

    def send_both(f, q):
        @pl.when(has_right)
        def _():
            to_right(f, z, q).start()

        @pl.when(has_left)
        def _():
            to_left(f, z, q).start()

    swaps = [
        send(spare.at[pl.ds(q * (cap // 2), cap // 2)], tok_part(y, z, q), swap_send.at[q], tok_recv.at[y, z, q],
             at(i, z, yo))
        for q in range(2)
    ]
    for q in range(2):
        swaps[q].start()
        send_both(y, q)
    slot_sends = []

    def send_slots(f, ii, q, device):
        block = slot_part(f, ii, q)
        copy = send(block, block, slot_send.at[len(slot_sends)], slot_recv.at[f, ii, q], device)
        copy.start()
        slot_sends.append(copy)

    loads[2].wait()
    for device in (at(i2, z, y), at(i, z, yo), at(i1, z, y)):
        for q in range(2):
            send_slots(y, i, q, device)
    loads[3].wait()
    price_sends = [
        send(prices.at[i], prices.at[i], price_send.at[k], price_recv.at[i], at(ii, z, y))
        for k, ii in enumerate([i1, i2, i3])
    ]
    for copy in price_sends:
        copy.start()

    def relay(d, f, q):
        @pl.when(has_right & (z - d >= 0))
        def _():
            zb = lax.max(z - d, 0)
            tok_arrived(f, zb, q)
            to_right(f, zb, q).start()

        @pl.when(has_left & (z + d < lines))
        def _():
            zb = lax.min(z + d, lines - 1)
            tok_arrived(f, zb, q)
            to_left(f, zb, q).start()

    beside, across, over = at(i1, z, y), at(i2, z, y), at(i, z, yo)
    for q in range(2):
        tok_arrived(yo, z, q)
        send_both(yo, q)
        relay(1, y, q)
    slot_arrived(y, i2, 0)
    send_slots(y, i2, 0, beside)
    relay(1, yo, 0)
    slot_arrived(yo, i, 0)
    send_slots(yo, i, 0, across)
    send_slots(yo, i, 0, beside)
    slot_arrived(y, i2, 1)
    send_slots(y, i2, 1, over)
    send_slots(y, i2, 1, beside)
    relay(1, yo, 1)
    if lines > 3:
        for q in range(2):
            relay(2, y, q)
    slot_arrived(yo, i, 1)
    send_slots(yo, i, 1, beside)
    if lines > 3:
        for q in range(2):
            relay(2, yo, q)

        def relay_all(d):
            for f in (y, yo):
                for q in range(2):
                    relay(d, f, q)

        loop(3, lines - 1, relay_all)
    for ii in (i1, i2, i3):
        arrived(prices.at[ii], price_recv.at[ii])
    for k in range(GROUP):
        column = column_of(prices[k].astype(jnp.float32) * unit_price, own)
        cost[k * own:(k + 1) * own] = jnp.broadcast_to(column, (own, cap))
    for q in range(2):
        slot_arrived(yo, i2, q)
        send_slots(yo, i2, q, beside)
    for f, ii in [(y, i1), (y, i3), (yo, i1), (yo, i3)]:
        for q in range(2):
            slot_arrived(f, ii, q)

    def score(zb, late=None):
        total = None
        for f in (y, yo):
            if late is not None:
                @pl.when(late)
                def _():
                    for q in range(2):
                        tok_arrived(f, zb, q)

            rows = slot[f].reshape(GROUP * own, slot.shape[3])
            part = lax.dot_general(
                rows, toks[f, zb], (((1,), (1,)), ((), ())), preferred_element_type=jnp.float32
            )
            total = part if total is None else total + part
        v = total - cost[...]
        vals[zb] = v
        step = 32
        b, s = v[:step], jnp.full((step, cap), -jnp.inf)
        for k in range(1, GROUP * own // step):
            row = v[step * k:step * (k + 1)]
            s = jnp.maximum(s, jnp.minimum(b, row))
            b = jnp.maximum(b, row)
        while step > 8:
            step //= 2
            b, s = keep_two((b[:step], s[:step]), (b[step:], s[step:]))
        for shift in (4, 2, 1):
            b, s = keep_two((b, s), (pltpu.roll(b, shift, 0), pltpu.roll(s, shift, 0)))
        stats[z, pl.ds(zb, 1)] = jnp.concatenate([b[0:1], s[0:1]], axis=1)

    score(z)

    def score_at(d):
        @pl.when(z - d >= 0)
        def _():
            zb = lax.max(z - d, 0)

            score(zb, jnp.logical_not(has_right))

        @pl.when(z + d < lines)
        def _():
            zb = lax.min(z + d, lines - 1)

            score(zb, jnp.logical_not(has_left))

    stats[z, lines:] = jnp.broadcast_to(busy, (lines, LANES))
    loop(1, lines, score_at)

    def stat_to(d):
        return send(stats.at[z], stats.at[z], stat_send.at[d], stat_recv.at[z], at(i, lax.rem(z + d, lines), y))

    loop(1, lines, lambda d: stat_to(d).start())

    def stat_arrived(d):
        zb = lax.rem(z + d, lines)
        arrived(stats.at[zb], stat_recv.at[zb])

    loop(1, lines, stat_arrived)
    b, s = stats[0, :lines, :cap], stats[0, :lines, cap:]
    for k in range(1, lines):
        b, s = keep_two((b, s), (stats[k, :lines, :cap], stats[k, :lines, cap:]))
    number = y * cap + iota((1, cap), 1)
    top, bidders = None, None
    for k in range(lines):
        count = stats[k, lines:lines + 1, :cap]
        valid = number.astype(jnp.float32) < count
        gaps[k] = jnp.where(valid, b[k:k + 1] - s[k:k + 1], 0.0)
        excess = vals[k] - jnp.where(valid, s[k:k + 1], jnp.inf)
        top = excess if top is None else jnp.maximum(top, excess)
        bidders = count if bidders is None else bidders + count
    bidders = bidders[:, :1]
    halves[y] = gaps[z]
    gap_to = send(halves.at[y], halves.at[y], gap_send, gap_recv, at(i, z, yo))
    gap_to.start()

    def raise_to(k):
        return send(outgoing.at[k], raises.at[here], raise_send.at[k], raise_recv.at[here],
                    at(k % GROUP, z, k // GROUP))

    for k in range(2 * GROUP):
        first = (k % GROUP) * own + (k // GROUP) * half
        column = jnp.max(top[first:first + half], axis=1, keepdims=True)
        shape = (half, LANES)
        row = jnp.max(jnp.where(iota(shape, 1) == iota(shape, 0), column, -jnp.inf), axis=0, keepdims=True)
        outgoing[k] = jnp.where(iota(row.shape, 1) == LANES - 1, bidders, row)

        @pl.when(here != k)
        def _():
            raise_to(k).start()

    raises[here] = outgoing[here]
    units = prices[i].astype(jnp.float32)
    own_prices = jnp.where(y == 0, units[:, :half], units[:, half:2 * half]) * unit_price

    arrived(halves.at[yo], gap_recv)
    both = jnp.concatenate([halves[0], halves[1]], axis=1)
    hit = where_to[...] == iota((2 * cap, own), 0).astype(jnp.float32)
    margins_out[...] = jnp.sum(jnp.where(hit, column_of(both, 2 * cap), 0.0), axis=0, keepdims=True)

    for ii, yy in plane:
        arrived(raises.at[yy * GROUP + ii], raise_recv.at[yy * GROUP + ii])
    highest, total = raises[0], raises[0]
    for k in range(1, 2 * GROUP):
        highest = jnp.maximum(highest, raises[k])
        total = total + raises[k]
    prices_out[...] = own_prices + jnp.maximum(highest[:, :half], 0.0)
    count_out[...] = (total[:, LANES - 1:] * 0.5).astype(jnp.int32)

    gap_to.wait_send()
    for copy in swaps + slot_sends + price_sends:
        copy.wait_send()
    loop(1, lines, lambda d: stat_to(d).wait_send())
    for k in range(2 * GROUP):
        @pl.when(here != k)
        def _():
            raise_to(k).wait_send()

    pieces = [(f, q) for f in range(2) for q in range(2)]

    def passed(zb):
        @pl.when(has_right & (zb <= z))
        def _():
            for f, q in pieces:
                to_right(f, zb, q).wait_send()

        @pl.when(has_left & (zb >= z))
        def _():
            for f, q in pieces:
                to_left(f, zb, q).wait_send()

    loop(0, lines, passed)


def on_device(tokens, slot_embed, price_units, unassigned):
    lines = lax.axis_size("dp") // GROUP
    own, width = tokens.shape
    half, cap = own // 2, BUSY // 2
    every = GROUP * own
    any_ = pl.BlockSpec(memory_space=pl.ANY)
    vmem = pl.BlockSpec(memory_space=pltpu.VMEM)
    dma = pltpu.SemaphoreType.DMA
    new_prices, margins, total = pl.pallas_call(
        functools.partial(kernel, lines, cap),
        out_shape=(
            pltpu.VMEM((1, half), jnp.float32),
            pltpu.VMEM((1, own), jnp.float32),
            pltpu.VMEM((1, 1), jnp.int32),
        ),
        in_specs=[any_] * 4,
        out_specs=(vmem,) * 3,
        scratch_shapes=[
            pltpu.VMEM((2, GROUP, own, width), jnp.bfloat16),
            pltpu.VMEM((2, lines, cap, width), jnp.bfloat16),
            pltpu.VMEM((own, width), jnp.bfloat16),
            pltpu.VMEM((cap, width), jnp.bfloat16),
            pltpu.VMEM((GROUP, 1, own), jnp.int32),
            pltpu.VMEM((1, own), jnp.int32),
            pltpu.VMEM((1, own), jnp.float32),
            pltpu.VMEM((every, cap), jnp.float32),
            pltpu.VMEM((lines, 2 * lines, LANES), jnp.float32),
            pltpu.VMEM((2 * GROUP, 1, LANES), jnp.float32),
            pltpu.VMEM((2 * GROUP, 1, LANES), jnp.float32),
            pltpu.VMEM((lines, every, cap), jnp.float32),
            pltpu.VMEM((lines, 1, cap), jnp.float32),
            pltpu.VMEM((2, 1, cap), jnp.float32),
            dma((4,)), dma((14,)), dma((2, GROUP, 2)), dma((2,)), dma((2, lines, 2)), dma((2, lines, 2)),
            dma((2, lines, 2)),
            dma((3,)), dma((GROUP,)), dma((lines,)), dma((lines,)), dma((2 * GROUP,)), dma((2 * GROUP,)), dma, dma,
        ],
        compiler_params=pltpu.CompilerParams(collective_id=0, has_side_effects=True),
        name="auction",
    )(tokens, slot_embed, price_units.reshape(1, -1), unassigned.reshape(1, -1))
    return new_prices.reshape(-1), margins.reshape(-1), total.reshape(())


def solution(mesh):
    return jax.shard_map(
        on_device,
        mesh=mesh,
        in_specs=(P("dp", "mp"), P("dp", "mp"), P("dp"), P("dp")),
        out_specs=(P(("dp", "mp")), P("dp"), P()),
        check_vma=False,
    )
```
